64 devices in a mesh: rep: 4 (over x, y), dp: 16 (over z, core).
Axes of the slice: x: 2, y: 2, z: 8, core: 2. Of those that a mesh axis runs over, the one named last changes fastest.
The devices are a block of a 4x4x8 slice.
Arguments:
- x: bfloat16 [64, 2048, 768], P(('rep', 'dp')), parts along dimension 0
- dy: bfloat16 [64, 2048, 768], P(('rep', 'dp')), parts along dimension 0
- w_gate: bfloat16 [2, 768, 2304], replicated
- w_up: bfloat16 [2, 768, 2304], replicated
- w_down: bfloat16 [2, 2304, 768], replicated
- m_w_gate: float32 [2, 768, 2304], P(None, 'dp')
- m_w_up: float32 [2, 768, 2304], P(None, 'dp')
- m_w_down: float32 [2, 2304, 768], P(None, 'dp')
- v_w_gate: float32 [2, 768, 2304], P(None, 'dp')
- v_w_up: float32 [2, 768, 2304], P(None, 'dp')
- v_w_down: float32 [2, 2304, 768], P(None, 'dp')
Outputs:
- output 1: bfloat16 [8, 768, 2304], P('rep'), parts along dimension 0
- output 2: bfloat16 [8, 768, 2304], P('rep'), parts along dimension 0
- output 3: bfloat16 [8, 2304, 768], P('rep'), parts along dimension 0
- output 4: float32 [8, 768, 2304], P('rep', 'dp'), parts along dimension 0
- output 5: float32 [8, 768, 2304], P('rep', 'dp'), parts along dimension 0
- output 6: float32 [8, 2304, 768], P('rep', 'dp'), parts along dimension 0
- output 7: float32 [8, 768, 2304], P('rep', 'dp'), parts along dimension 0
- output 8: float32 [8, 768, 2304], P('rep', 'dp'), parts along dimension 0
- output 9: float32 [8, 2304, 768], P('rep', 'dp'), parts along dimension 0
There are 4 independent parts. The reference program is written for one: setup_inputs(seed, part) draws one part's arguments, and reference() takes and returns one part's arrays. A program takes and returns all parts, laid end to end along the dimension named above; an argument that names none is the same for every part.
All inputs are finite; a program needn't handle non-finite values.
Results may differ from the reference program's by a relative error of at most 0.022.
Values are sent between devices in bfloat16 or wider.
A program may use at most 768 MiB of HBM per device.

```python
import jax
import jax.numpy as jnp
from jax import lax

SEQUENCES = 16
TOKENS = 2048
D = 768
FF = 2304
LAYERS = 2
NAMES = ("w_gate", "w_up", "w_down")
SHAPES = {"w_gate": (LAYERS, D, FF), "w_up": (LAYERS, D, FF), "w_down": (LAYERS, FF, D)}


def bump(key, n, height):
    away = (jnp.arange(n, dtype=jnp.int32) - jax.random.randint(key, (), 0, n, jnp.int32)) % n
    return jnp.where(away < n // 8, height, 1.0)


def together(key, own, strength):
    shared = jax.random.normal(key, own.shape[1:], jnp.float32)
    return (own + strength * shared) * lax.rsqrt(1 + strength * strength)


def setup_inputs(seed: int = 0, part: int = 0) -> dict:
    kx, kdy, ka, kb, kz, kf, kh, kl, *keys = jax.random.split(jax.random.key(seed), 8 + 3 * len(NAMES))
    kx, kdy, ka, kb = (jax.random.fold_in(k, part) for k in (kx, kdy, ka, kb))
    kw, km, kv = (keys[i::3] for i in range(3))
    shape = (SEQUENCES, TOKENS, D)
    much_x, much_dy = jax.random.uniform(kz, (2,), jnp.float32, 0.0, 1.0)
    loud = 2.0 ** jax.random.uniform(jax.random.fold_in(kz, 1), (), jnp.float32, -1.0, 2.0)
    layers = 2.0 ** jax.random.uniform(kl, (LAYERS, 1, 1), jnp.float32, -1.0, 1.0)
    x = together(ka, jax.random.normal(kx, shape, jnp.float32), much_x) * bump(kf, D, 4.0)
    dy = together(kb, jax.random.normal(kdy, shape, jnp.float32), much_dy)
    drawn = {"x": x.astype(jnp.bfloat16), "dy": (loud * dy * (SEQUENCES * TOKENS) ** -0.5).astype(jnp.bfloat16)}
    for key, name in zip(kw, NAMES, strict=True):
        w = jax.random.normal(key, SHAPES[name], jnp.float32) * SHAPES[name][1] ** -0.5
        drawn[name] = (w * {"w_gate": 1.0, "w_up": bump(kh, FF, 4.0), "w_down": layers}[name]).astype(jnp.bfloat16)
    for key, name in zip(km, NAMES, strict=True):
        drawn[f"m_{name}"] = 0.1 * jax.random.normal(key, SHAPES[name], jnp.float32)
    for key, name in zip(kv, NAMES, strict=True):
        drawn[f"v_{name}"] = jax.random.uniform(key, SHAPES[name], jnp.float32, 0.005, 0.015)
    return drawn


def matmul(a, w):
    return jnp.dot(a, w, preferred_element_type=jnp.float32).astype(jnp.bfloat16)


def normed(h):
    wide = h.astype(jnp.float32)
    scale = lax.rsqrt(jnp.mean(wide**2, -1, keepdims=True) + 1e-6)
    return (wide * scale).astype(jnp.bfloat16)


def layer(h, w):
    a = normed(h)
    gate = jnp.dot(a, w["w_gate"], preferred_element_type=jnp.float32)
    up = jnp.dot(a, w["w_up"], preferred_element_type=jnp.float32)
    return h + matmul((jax.nn.silu(gate) * up).astype(jnp.bfloat16), w["w_down"])


def adamw(w, m, v, g):
    m = 0.9 * m + 0.1 * g
    v = 0.95 * v + 0.05 * g * g
    step = m * lax.rsqrt(v + 1e-8) + 0.1 * w
    return (w - 0.02 * step).astype(jnp.bfloat16), m, v


def stack(weights, h):
    return lax.scan(lambda h, w: (layer(h, w), None), h, weights)[0]


def reference(x, dy, w_gate, w_up, w_down, m_w_gate, m_w_up, m_w_down, v_w_gate, v_w_up, v_w_down):
    weights = dict(zip(NAMES, (w_gate, w_up, w_down), strict=True))

    def take(so_far, sequence):
        h, by_y = sequence
        _, back = jax.vjp(lambda w: stack(w, h), weights)
        return jax.tree.map(lambda total, term: total + term.astype(jnp.float32), so_far, back(by_y)[0]), None

    none_yet = {name: jnp.zeros(w.shape, jnp.float32) for name, w in weights.items()}
    by_weights, _ = lax.scan(take, none_yet, (x, dy))
    gradients = [by_weights[name].astype(jnp.bfloat16).astype(jnp.float32) for name in NAMES]
    new = [
        adamw(w.astype(jnp.float32), m, v, g)
        for w, m, v, g in zip((w_gate, w_up, w_down), (m_w_gate, m_w_up, m_w_down), (v_w_gate, v_w_up, v_w_down), gradients, strict=True)
    ]
    return tuple(one[which] for which in range(3) for one in new)
```

```python
import functools

import jax
import jax.numpy as jnp
from jax import lax
from jax.experimental import pallas as pl
from jax.experimental.pallas import tpu as pltpu
from jax.sharding import PartitionSpec as P

CORES = 2
F32, BF16 = jnp.float32, jnp.bfloat16
VMEM_LIMIT = 67_043_328


def dot(a, b):
    return lax.dot_general(a, b, (((1,), (0,)), ((), ())), preferred_element_type=F32)


def dot_nt(a, b):
    return lax.dot_general(a, b, (((1,), (1,)), ((), ())), preferred_element_type=F32)


def chain_kernel(layers, blocks, x_ref, dy_ref, wg_ref, wu_ref, wd_ref, left_ref, right_ref):
    d = x_ref.shape[1]
    per = wg_ref.shape[2] // d
    rows = d // blocks
    h = x_ref[...]
    saved = []
    for l in range(layers):
        wide = h.astype(F32)
        scale = lax.rsqrt(jnp.mean(wide * wide, -1, keepdims=True) + 1e-6)
        a = wide * scale
        left_ref[l, per] = a.T.astype(BF16)
        a = a.astype(BF16)
        gate = dot(a, wg_ref[l])
        up = dot(a, wu_ref[l])
        act = jax.nn.sigmoid(gate) * gate * up
        turned = act.T.astype(BF16)
        for j in range(blocks):
            for c in range(per):
                left_ref[l, c, j * rows : (j + 1) * rows, :] = turned[(j * per + c) * rows : (j * per + c + 1) * rows, :]
        saved.append((wide, scale, gate, up))
        if l < layers - 1:
            h = (wide + dot(act.astype(BF16), wd_ref[l]).astype(BF16).astype(F32)).astype(BF16)
    dh = dy_ref[...]
    for l in reversed(range(layers)):
        wide, scale, gate, up = saved[l]
        right_ref[l, 0] = dh
        dact = dot_nt(dh, wd_ref[l]).astype(BF16).astype(F32)
        sig = jax.nn.sigmoid(gate)
        silu = gate * sig
        dup = (dact * silu).astype(BF16)
        dgate = (dact * up * (sig + silu * (1.0 - sig))).astype(BF16)
        for c in range(per):
            right_ref[l, 1 + c] = dgate[:, c * d : (c + 1) * d]
            right_ref[l, 1 + per + c] = dup[:, c * d : (c + 1) * d]
        if l > 0:
            da = (dot_nt(dgate, wg_ref[l]) + dot_nt(dup, wu_ref[l])).astype(BF16).astype(F32)
            mean = jnp.mean(wide * da, -1, keepdims=True)
            dwide = da * scale - wide * (scale * scale * scale * mean)
            dh = (dh.astype(F32) + dwide.astype(BF16).astype(F32)).astype(BF16)


def chain(x, dy, wg, wu, wd, blocks, tile):
    layers, d, ff = wg.shape
    tokens = x.shape[0]
    per = ff // d
    whole = pl.BlockSpec(memory_space=pltpu.VMEM)
    tokens_by = pl.BlockSpec((tile, d), lambda t: (t, 0))
    return pl.pallas_call(
        functools.partial(chain_kernel, layers, blocks),
        grid=(tokens // tile,),
        in_specs=[tokens_by, tokens_by, whole, whole, whole],
        out_specs=[
            pl.BlockSpec((layers, per + 1, d, tile), lambda t: (0, 0, 0, t)),
            pl.BlockSpec((layers, 2 * per + 1, tile, d), lambda t: (0, 0, t, 0)),
        ],
        out_shape=[
            jax.ShapeDtypeStruct((layers, per + 1, d, tokens), BF16),
            jax.ShapeDtypeStruct((layers, 2 * per + 1, tokens, d), BF16),
        ],
        compiler_params=pltpu.CompilerParams(vmem_limit_bytes=VMEM_LIMIT, dimension_semantics=("arbitrary",)),
        name="chain",
    )(x, dy, wg, wu, wd)


def exchange_kernel(n, layers, per, wide, slots, *refs):
    (left_hbm, right_hbm, wd_hbm, wg_hbm, wu_hbm, *rest) = refs
    m_in, v_in, new_hbm, m_out, v_out = rest[0:3], rest[3:6], rest[6], rest[7:10], rest[10:13]
    (lbuf, rbuf, own, pair, got, w_rows, w_new, load_sem, w_sem, pair_send, pair_recv, sum_send, sum_recv,
     ring_send, ring_recv, side_send, side_recv, keep_sem) = rest[13:]
    weights = (wd_hbm, wg_hbm, wu_hbm)
    chips = n // CORES
    far = chips // 2
    near = chips - 1 - far
    d = rbuf.shape[2]
    rows = d // n
    per_layer = 3 * per
    chunks = layers * per_layer
    me = lax.axis_index("dp")
    z, k = lax.div(me, CORES), lax.rem(me, CORES)
    sign = 1 - 2 * k
    at = lambda chip: {"dp": lax.rem(chip + 2 * chips, chips) * CORES + k}
    place = lambda chip: lax.rem(chip + 2 * chips, chips)
    fore, back, mate = at(z + sign), at(z - sign), {"dp": z * CORES + 1 - k}

    def split(i):
        layer = layers - 1 - lax.div(i, per_layer)
        q = lax.rem(i, per_layer)
        kind = lax.div(q, per)
        inner = lax.div(kind + 1, 2)
        return layer, kind, lax.rem(q, per), (1 - inner) * q + inner * per, inner * (q - per + 1)

    def loads(i):
        layer, _, _, of_left, of_right = split(i)
        s = lax.rem(i, 2)
        return (
            pltpu.make_async_copy(left_hbm.at[layer, of_left], lbuf.at[s], load_sem.at[s, 0]),
            pltpu.make_async_copy(right_hbm.at[layer, of_right], rbuf.at[s], load_sem.at[s, 1]),
        )

    def remote(src, dst, send, recv, device):
        return pltpu.make_async_remote_copy(
            src_ref=src, dst_ref=dst, send_sem=send, recv_sem=recv, device_id=device, device_id_type=pl.DeviceIdType.MESH
        )

    def w_loads():
        return [
            pltpu.make_async_copy(w.at[:, pl.ds(pl.multiple_of(me * r.shape[1], rows), r.shape[1]), :], r, w_sem.at[j])
            for j, (w, r) in enumerate(zip(weights, w_rows, strict=True))
        ]

    for copy in loads(0):
        copy.start()
    for copy in w_loads():
        copy.start()
    barrier = pltpu.get_barrier_semaphore()
    for device in (fore, back, mate):
        pl.semaphore_signal(barrier, inc=1, device_id=device, device_id_type=pl.DeviceIdType.MESH)
    pl.semaphore_wait(barrier, 3)
    for copy in w_loads():
        copy.wait()

    def to_mate(i):
        return remote(own.at[lax.rem(i, slots), 1 - k], pair.at[i], pair_send.at[i], pair_recv.at[i], mate)

    def far_sum(i, s):
        return remote(pair.at[i, place(z - sign * (far - s))], got.at[i, s], sum_send.at[i, s], sum_recv.at[i, s], back)

    def near_sum(i, s):
        j = far + s
        return remote(pair.at[i, place(z + sign * (near - s))], got.at[i, j], sum_send.at[i, j], sum_recv.at[i, j], fore)

    def block(i, chip, core):
        return new_hbm.at[i, place(chip) * CORES + core]

    def far_ring(i, s):
        src = w_new.at[i] if s == 0 else block(i, z - sign * s, k)
        return remote(src, block(i, z - sign * s, k), ring_send.at[i, s], ring_recv.at[i, s], fore)

    def near_ring(i, s):
        src = w_new.at[i] if s == 0 else block(i, z + sign * s, k)
        return remote(src, block(i, z + sign * s, k), ring_send.at[i, far + s], ring_recv.at[i, far + s], back)

    def far_came(i, s):
        dst = block(i, z - sign * (s + 1), k)
        return remote(dst, dst, ring_send.at[i, s], ring_recv.at[i, s], fore)

    def near_came(i, s):
        dst = block(i, z + sign * (s + 1), k)
        return remote(dst, dst, ring_send.at[i, far + s], ring_recv.at[i, far + s], back)

    def side(i, j):
        offset = 0 if j == 0 else (-j if j <= far else j - far)
        src = w_new.at[i] if j == 0 else block(i, z + sign * offset, k)
        return remote(src, block(i, z + sign * offset, k), side_send.at[i, j], side_recv.at[i, j], mate)

    def side_came(i, j):
        offset = 0 if j == 0 else (-j if j <= far else j - far)
        dst = block(i, z - sign * offset, 1 - k)
        return remote(dst, dst, side_send.at[i, j], side_recv.at[i, j], mate)

    def keep(i):
        return pltpu.make_async_copy(w_new.at[i], block(i, z, k), keep_sem.at[i])

    def multiply(i):
        s, slot = lax.rem(i, 2), lax.rem(i, slots)

        @pl.when(i + 1 < chunks)
        def _():
            for copy in loads(i + 1):
                copy.start()

        for copy in loads(i):
            copy.wait()

        def columns(c, _):
            cut = pl.ds(pl.multiple_of(c * wide, wide), wide)
            out = dot(lbuf[s], rbuf[s, :, cut]).astype(BF16).reshape(chips, CORES, rows, wide)
            for core in range(CORES):
                own[slot, core, :, :, cut] = out[:, core]
            return 0

        lax.fori_loop(0, d // wide, columns, 0)
        to_mate(i).start()

    def total(i, chip, *others):
        j = place(chip)
        out = own[lax.rem(i, slots), k, j].astype(F32) + pair[i, j].astype(F32)
        for other in others:
            out = out + got[i, other].astype(F32)
        return out.astype(BF16)

    def first(i):
        to_mate(i).wait()
        pair[i, place(z - sign * far)] = total(i, z - sign * far)
        far_sum(i, 0).start()
        pair[i, place(z + sign * near)] = total(i, z + sign * near)
        near_sum(i, 0).start()

    def onward(s, i):
        far_sum(i, s - 1).wait_recv()
        pair[i, place(z - sign * (far - s))] = total(i, z - sign * (far - s), s - 1)
        far_sum(i, s).start()
        if s < near:
            near_sum(i, s - 1).wait_recv()
            pair[i, place(z + sign * (near - s))] = total(i, z + sign * (near - s), far + s - 1)
            near_sum(i, s).start()

    def update(i):
        far_sum(i, far - 1).wait_recv()
        near_sum(i, near - 1).wait_recv()
        g = total(i, z, far - 1, far + near - 1).astype(F32)
        layer, kind, part, _, _ = split(i)
        for which in range(3):

            @pl.when(kind == which)
            def _(which=which):
                if which == 0:
                    cut = (layer, pl.ds(pl.multiple_of(part * rows, rows), rows), slice(None))
                else:
                    cut = (layer, slice(None), pl.ds(pl.multiple_of(part * d, d), d))
                w = w_rows[which][cut].astype(F32)
                m = 0.9 * m_in[which][cut] + 0.1 * g
                v = 0.95 * v_in[which][cut] + 0.05 * g * g
                m_out[which][cut] = m
                v_out[which][cut] = v
                w_new[i] = (w - 0.02 * (m * lax.rsqrt(v + 1e-8) + 0.1 * w)).astype(BF16)

        far_ring(i, 0).start()
        near_ring(i, 0).start()
        side(i, 0).start()
        keep(i).start()

    def gather(s, i):
        far_came(i, s - 1).wait_recv()
        if s < far:
            far_ring(i, s).start()
        side(i, s).start()
        if s <= near:
            near_came(i, s - 1).wait_recv()
            if s < near:
                near_ring(i, s).start()
            side(i, far + s).start()

    def drain(i):
        for s in range(far):
            far_sum(i, s).wait_send()
            far_ring(i, s).wait_send()
        for s in range(near):
            near_sum(i, s).wait_send()
            near_ring(i, s).wait_send()
        for j in range(chips):
            side(i, j).wait_send()
            side_came(i, j).wait_recv()
        keep(i).wait()

    stages = [multiply, first]
    stages += [functools.partial(onward, s) for s in range(1, far)]
    stages += [update]
    stages += [functools.partial(gather, s) for s in range(1, far + 1)]
    stages += [drain]

    def tick(t, _):
        for offset in reversed(range(len(stages))):
            i = t - offset

            @pl.when((i >= 0) & (i < chunks))
            def _(i=i, stage=stages[offset]):
                stage(i)

        return 0

    lax.fori_loop(0, chunks + len(stages) - 1, tick, 0)


def exchange(left, right, weights, m, v, n):
    layers, _, d, tokens = left.shape
    per = left.shape[1] - 1
    rows = d // n
    chips = n // CORES
    hops = chips - 1
    chunks = layers * 3 * per
    stages = 4 + 2 * (chips // 2)
    slots = 2 + chips // 2 + 1
    wide = 256 if d % 256 == 0 else d
    anywhere, vmem = pl.BlockSpec(memory_space=pl.ANY), pl.BlockSpec(memory_space=pltpu.VMEM)
    sems = lambda *shape: pltpu.SemaphoreType.DMA(shape)
    return pl.pallas_call(
        functools.partial(exchange_kernel, n, layers, per, wide, slots),
        in_specs=[anywhere] * 5 + [vmem] * 6,
        out_specs=[anywhere] + [vmem] * 6,
        out_shape=[jax.ShapeDtypeStruct((chunks, n, rows, d), BF16), *(jax.ShapeDtypeStruct(t.shape, F32) for t in (*m, *v))],
        scratch_shapes=[
            pltpu.VMEM((2, d, tokens), BF16),
            pltpu.VMEM((2, tokens, d), BF16),
            pltpu.VMEM((slots, CORES, chips, rows, d), BF16),
            pltpu.VMEM((chunks, chips, rows, d), BF16),
            pltpu.VMEM((chunks, hops, rows, d), BF16),
            [pltpu.VMEM(t.shape, BF16) for t in m],
            pltpu.VMEM((chunks, rows, d), BF16),
            sems(2, 2),
            sems(3),
            sems(chunks),
            sems(chunks),
            sems(chunks, hops),
            sems(chunks, hops),
            sems(chunks, hops),
            sems(chunks, hops),
            sems(chunks, chips),
            sems(chunks, chips),
            sems(chunks),
        ],
        compiler_params=pltpu.CompilerParams(collective_id=0, has_side_effects=True, vmem_limit_bytes=VMEM_LIMIT),
        name="exchange",
    )(left, right, *weights, *m, *v)


def solution(mesh):
    n = mesh.shape["dp"]

    def of_a_device(x, dy, wg, wu, wd, mg, mu, md, vg, vu, vd):
        layers, d, ff = wg.shape
        per = ff // d
        tokens = x.shape[1]
        left, right = chain(x[0], dy[0], wg, wu, wd, n, min(tokens, 256))
        new, nmd, nmg, nmu, nvd, nvg, nvu = exchange(left, right, (wd, wg, wu), (md, mg, mu), (vd, vg, vu), n)
        new = new.reshape(layers, 3, per, n, d // n, d)[::-1]
        wide = lambda t: t.transpose(0, 2, 3, 1, 4).reshape(layers, d, ff)
        down = new[:, 0].transpose(0, 2, 1, 3, 4).reshape(layers, ff, d)
        return wide(new[:, 1]), wide(new[:, 2]), down, nmg, nmu, nmd, nvg, nvu, nvd

    data, whole, part, groups, both = P(("rep", "dp")), P(), P(None, "dp"), P("rep"), P("rep", "dp")
    return jax.shard_map(
        of_a_device,
        mesh=mesh,
        in_specs=(data, data, *[whole] * 3, *[part] * 6),
        out_specs=(*[groups] * 3, *[both] * 6),
        check_vma=False,
    )
```

```python
import functools

import jax
import jax.numpy as jnp
from jax import lax
from jax.experimental import pallas as pl
from jax.experimental.pallas import tpu as pltpu
from jax.sharding import PartitionSpec as P

CORES = 2
F32, BF16 = jnp.float32, jnp.bfloat16
VMEM_LIMIT = 67_043_328


def dot(a, b):
    return lax.dot_general(a, b, (((1,), (0,)), ((), ())), preferred_element_type=F32)


def dot_nt(a, b):
    return lax.dot_general(a, b, (((1,), (1,)), ((), ())), preferred_element_type=F32)


def silu_back(gate, up, dact):
    sig = jax.nn.sigmoid(gate)
    silu = gate * sig
    return (dact * up * (sig + silu * (1.0 - sig))).astype(BF16), (dact * silu).astype(BF16)


def adamw(w, m, v, g):
    m = 0.9 * m + 0.1 * g
    v = 0.95 * v + 0.05 * g * g
    return (w - 0.02 * (m * lax.rsqrt(v + 1e-8) + 0.1 * w)).astype(BF16), m, v


def chain_kernel(layers, blocks, x_ref, dy_ref, wg_ref, wu_ref, wd_ref, left_ref, right_ref, low_ref, h_ref):
    d = x_ref.shape[1]
    per = wg_ref.shape[2] // d
    rows = d // blocks
    h = x_ref[...]
    for l in range(layers):
        wide = h.astype(F32)
        scale = lax.rsqrt(jnp.mean(wide * wide, -1, keepdims=True) + 1e-6)
        a = wide * scale
        left_ref[l, per] = a.T.astype(BF16)
        a = a.astype(BF16)
        gate = dot(a, wg_ref[l])
        up = dot(a, wu_ref[l])
        act = jax.nn.sigmoid(gate) * gate * up
        turned = act.T.astype(BF16)
        for j in range(blocks):
            for c in range(per):
                left_ref[l, c, j * rows : (j + 1) * rows, :] = turned[(j * per + c) * rows : (j * per + c + 1) * rows, :]
        if l < layers - 1:
            for c in range(per):
                low_ref[0, c] = gate[:, c * d : (c + 1) * d]
                low_ref[1, c] = up[:, c * d : (c + 1) * d]
            h = (wide + dot(act.astype(BF16), wd_ref[l]).astype(BF16).astype(F32)).astype(BF16)
            h_ref[...] = h
    dh = dy_ref[...]
    right_ref[0] = dh
    dgate, dup = silu_back(gate, up, dot_nt(dh, wd_ref[layers - 1]).astype(BF16).astype(F32))
    for c in range(per):
        right_ref[1 + c] = dgate[:, c * d : (c + 1) * d]
        right_ref[1 + per + c] = dup[:, c * d : (c + 1) * d]


def chain(x, dy, wg, wu, wd, blocks, tile):
    layers, d, ff = wg.shape
    tokens = x.shape[0]
    per = ff // d
    whole = pl.BlockSpec(memory_space=pltpu.VMEM)
    tokens_by = pl.BlockSpec((tile, d), lambda t: (t, 0))
    return pl.pallas_call(
        functools.partial(chain_kernel, layers, blocks),
        grid=(tokens // tile,),
        in_specs=[tokens_by, tokens_by, whole, whole, whole],
        out_specs=[
            pl.BlockSpec((layers, per + 1, d, tile), lambda t: (0, 0, 0, t)),
            pl.BlockSpec((2 * per + 1, tile, d), lambda t: (0, t, 0)),
            pl.BlockSpec((2, per, tile, d), lambda t: (0, 0, t, 0)),
            tokens_by,
        ],
        out_shape=[
            jax.ShapeDtypeStruct((layers, per + 1, d, tokens), BF16),
            jax.ShapeDtypeStruct((2 * per + 1, tokens, d), BF16),
            jax.ShapeDtypeStruct((2, per, tokens, d), F32),
            jax.ShapeDtypeStruct((tokens, d), BF16),
        ],
        compiler_params=pltpu.CompilerParams(vmem_limit_bytes=VMEM_LIMIT, dimension_semantics=("arbitrary",)),
        name="chain",
    )(x, dy, wg, wu, wd)


def exchange_kernel(n, layers, per, wide, slots, tile, early, *refs):
    (left_hbm, top_hbm, low_hbm, h_hbm, wd_hbm, wg_hbm, wu_hbm, *rest) = refs
    m_hbm, v_hbm, new_hbm, g_out, right_hbm = rest[0:3], rest[3:6], rest[6], rest[7], rest[8]
    (lbuf, rbuf, own, pair, got, state, w_new, w_tile, t_tile, g_tile, s_tile, load_sem, state_sem, pair_send, pair_recv,
     sum_send, sum_recv, ring_send, ring_recv, side_send, side_recv, keep_sem, w_sem, in_sem, out_sem) = rest[9:]
    weights = (wd_hbm, wg_hbm, wu_hbm)
    chips = n // CORES
    far = chips // 2
    near = chips - 1 - far
    d = rbuf.shape[2]
    rows = d // n
    per_layer = 3 * per
    chunks = layers * per_layer
    me = lax.axis_index("dp")
    z, k = lax.div(me, CORES), lax.rem(me, CORES)
    sign = 1 - 2 * k
    at = lambda chip: {"dp": lax.rem(chip + 2 * chips, chips) * CORES + k}
    place = lambda chip: lax.rem(chip + 2 * chips, chips)
    fore, back, mate = at(z + sign), at(z - sign), {"dp": z * CORES + 1 - k}

    def split(i):
        layer = layers - 1 - lax.div(i, per_layer)
        q = lax.rem(i, per_layer)
        kind = lax.div(q, per)
        inner = lax.div(kind + 1, 2)
        return layer, kind, lax.rem(q, per), (1 - inner) * q + inner * per, inner * (q - per + 1)

    def start_loads(i):
        layer, _, _, of_left, of_right = split(i)
        s = lax.rem(i, 2)
        pltpu.make_async_copy(left_hbm.at[layer, of_left], lbuf.at[s], load_sem.at[s, 0]).start()
        for low, right in enumerate((top_hbm, right_hbm)):

            @pl.when((i >= per_layer) == (low == 1))
            def _(right=right):
                pltpu.make_async_copy(right.at[of_right], rbuf.at[s], load_sem.at[s, 1]).start()

    def wait_loads(i):
        s = lax.rem(i, 2)
        pltpu.make_async_copy(left_hbm.at[0, 0], lbuf.at[s], load_sem.at[s, 0]).wait()
        pltpu.make_async_copy(top_hbm.at[0], rbuf.at[s], load_sem.at[s, 1]).wait()

    def start_state(i):
        layer, kind, part, _, _ = split(i)
        s = lax.rem(i, 2)
        for which in range(3):

            @pl.when(kind == which)
            def _(which=which):
                if which == 0:
                    first_row = pl.multiple_of(me * (per * rows) + part * rows, rows)
                    w_cut = (layer, pl.ds(first_row, rows), slice(None))
                    cut = (layer, pl.ds(pl.multiple_of(part * rows, rows), rows), slice(None))
                else:
                    columns = pl.ds(pl.multiple_of(part * d, d), d)
                    w_cut = (layer, pl.ds(pl.multiple_of(me * rows, rows), rows), columns)
                    cut = (layer, slice(None), columns)
                pltpu.make_async_copy(weights[which].at[w_cut], w_new.at[i], state_sem.at[s, 0]).start()
                pltpu.make_async_copy(m_hbm[which].at[cut], state.at[s, 0], state_sem.at[s, 1]).start()
                pltpu.make_async_copy(v_hbm[which].at[cut], state.at[s, 1], state_sem.at[s, 2]).start()

    def wait_state(i):
        s = lax.rem(i, 2)
        pltpu.make_async_copy(wg_hbm.at[0, 0:rows, 0:d], w_new.at[i], state_sem.at[s, 0]).wait()
        for j, moment in enumerate((m_hbm[1], v_hbm[1])):
            pltpu.make_async_copy(moment.at[0, :, 0:d], state.at[s, j], state_sem.at[s, 1 + j]).wait()

    def remote(src, dst, send, recv, device):
        return pltpu.make_async_remote_copy(
            src_ref=src, dst_ref=dst, send_sem=send, recv_sem=recv, device_id=device, device_id_type=pl.DeviceIdType.MESH
        )

    tiles = top_hbm.shape[1] // tile

    def tokens_of(e):
        return pl.ds(pl.multiple_of(lax.rem(e, tiles) * tile, tile), tile)

    def top_weights():
        return [
            pltpu.make_async_copy(w.at[layers - 1, :, c * d : (c + 1) * d], w_tile.at[j * per + c], w_sem.at[j * per + c])
            for j, w in enumerate((wg_hbm, wu_hbm))
            for c in range(per)
        ]

    def low_weights():
        return [pltpu.make_async_copy(wd_hbm.at[0, c * d : (c + 1) * d, :], w_tile.at[c], w_sem.at[c]) for c in range(per)]

    def top_inputs(e):
        cut = tokens_of(e)
        return (
            pltpu.make_async_copy(top_hbm.at[1:, cut, :], t_tile, in_sem.at[0]),
            pltpu.make_async_copy(top_hbm.at[0, cut, :], s_tile.at[0], in_sem.at[1]),
            pltpu.make_async_copy(h_hbm.at[cut, :], s_tile.at[1], in_sem.at[2]),
        )

    def low_inputs(e):
        cut = tokens_of(e)
        return (
            pltpu.make_async_copy(low_hbm.at[:, :, cut, :], g_tile, in_sem.at[3]),
            pltpu.make_async_copy(right_hbm.at[0, cut, :], s_tile.at[0], in_sem.at[1]),
        )

    def top_result(e):
        return pltpu.make_async_copy(s_tile.at[2], right_hbm.at[0, tokens_of(e), :], out_sem.at[0])

    def low_result(e):
        return pltpu.make_async_copy(t_tile, right_hbm.at[1:, tokens_of(e), :], out_sem.at[1])

    def extra(e):
        @pl.when((e >= 0) & (e < tiles))
        def _():
            @pl.when(e == 0)
            def _():
                for copy in top_weights():
                    copy.wait()

            @pl.when(e > 0)
            def _():
                top_result(e - 1).wait()

            for copy in top_inputs(e):
                copy.wait()
            da = dot_nt(t_tile[0], w_tile[0])
            for c in range(1, 2 * per):
                da = da + dot_nt(t_tile[c], w_tile[c])
            da = da.astype(BF16).astype(F32)
            wide = s_tile[1].astype(F32)
            scale = lax.rsqrt(jnp.mean(wide * wide, -1, keepdims=True) + 1e-6)
            mean = jnp.mean(wide * da, -1, keepdims=True)
            dwide = da * scale - wide * (scale * scale * scale * mean)
            s_tile[2] = (s_tile[0].astype(F32) + dwide.astype(BF16).astype(F32)).astype(BF16)
            top_result(e).start()

            @pl.when(e < tiles - 1)
            def _():
                for copy in top_inputs(e + 1):
                    copy.start()

            @pl.when(e == tiles - 1)
            def _():
                for copy in (*low_weights(), *low_inputs(e + 1)):
                    copy.start()

        @pl.when((e >= tiles) & (e < 2 * tiles))
        def _():
            @pl.when(e == tiles)
            def _():
                top_result(e - 1).wait()
                for copy in low_weights():
                    copy.wait()

            @pl.when(e > tiles)
            def _():
                low_result(e - 1).wait()

            for copy in low_inputs(e):
                copy.wait()
            for c in range(per):
                dact = dot_nt(s_tile[0], w_tile[c]).astype(BF16).astype(F32)
                t_tile[c], t_tile[per + c] = silu_back(g_tile[0, c], g_tile[1, c], dact)
            low_result(e).start()

            @pl.when(e < 2 * tiles - 1)
            def _():
                for copy in low_inputs(e + 1):
                    copy.start()

        @pl.when(e == 2 * tiles)
        def _():
            low_result(e - 1).wait()

    start_loads(0)
    for copy in (*top_weights(), *top_inputs(0)):
        copy.start()
    barrier = pltpu.get_barrier_semaphore()
    for device in (fore, back, mate):
        pl.semaphore_signal(barrier, inc=1, device_id=device, device_id_type=pl.DeviceIdType.MESH)
    pl.semaphore_wait(barrier, 3)

    def to_mate(i):
        return remote(own.at[lax.rem(i, slots), 1 - k], pair.at[i], pair_send.at[i], pair_recv.at[i], mate)

    def far_sum(i, s):
        return remote(pair.at[i, place(z - sign * (far - s))], got.at[i, s], sum_send.at[i, s], sum_recv.at[i, s], back)

    def near_sum(i, s):
        j = far + s
        return remote(pair.at[i, place(z + sign * (near - s))], got.at[i, j], sum_send.at[i, j], sum_recv.at[i, j], fore)

    def block(i, chip, core):
        return new_hbm.at[i, place(chip) * CORES + core]

    def far_ring(i, s):
        src = w_new.at[i] if s == 0 else block(i, z - sign * s, k)
        return remote(src, block(i, z - sign * s, k), ring_send.at[i, s], ring_recv.at[i, s], fore)

    def near_ring(i, s):
        src = w_new.at[i] if s == 0 else block(i, z + sign * s, k)
        return remote(src, block(i, z + sign * s, k), ring_send.at[i, far + s], ring_recv.at[i, far + s], back)

    def far_came(i, s):
        dst = block(i, z - sign * (s + 1), k)
        return remote(dst, dst, ring_send.at[i, s], ring_recv.at[i, s], fore)

    def near_came(i, s):
        dst = block(i, z + sign * (s + 1), k)
        return remote(dst, dst, ring_send.at[i, far + s], ring_recv.at[i, far + s], back)

    def side(i, j):
        offset = 0 if j == 0 else (-j if j <= far else j - far)
        src = w_new.at[i] if j == 0 else block(i, z + sign * offset, k)
        return remote(src, block(i, z + sign * offset, k), side_send.at[i, j], side_recv.at[i, j], mate)

    def side_came(i, j):
        offset = 0 if j == 0 else (-j if j <= far else j - far)
        dst = block(i, z - sign * offset, 1 - k)
        return remote(dst, dst, side_send.at[i, j], side_recv.at[i, j], mate)

    def keep(i):
        return pltpu.make_async_copy(w_new.at[i], block(i, z, k), keep_sem.at[i])

    def multiply(i):
        s, slot = lax.rem(i, 2), lax.rem(i, slots)

        @pl.when(i + 1 < chunks)
        def _():
            start_loads(i + 1)

        wait_loads(i)

        def columns(c, _):
            cut = pl.ds(pl.multiple_of(c * wide, wide), wide)
            out = dot(lbuf[s], rbuf[s, :, cut]).astype(BF16).reshape(chips, CORES, rows, wide)
            for core in range(CORES):
                own[slot, core, :, :, cut] = out[:, core]
            return 0

        lax.fori_loop(0, d // wide, columns, 0)
        to_mate(i).start()

    def total(i, chip, *others):
        j = place(chip)
        out = own[lax.rem(i, slots), k, j].astype(F32) + pair[i, j].astype(F32)
        for other in others:
            out = out + got[i, other].astype(F32)
        return out.astype(BF16)

    def first(i):
        to_mate(i).wait()
        pair[i, place(z - sign * far)] = total(i, z - sign * far)
        far_sum(i, 0).start()
        pair[i, place(z + sign * near)] = total(i, z + sign * near)
        near_sum(i, 0).start()

    def onward(s, i):
        far_sum(i, s - 1).wait_recv()
        pair[i, place(z - sign * (far - s))] = total(i, z - sign * (far - s), s - 1)
        far_sum(i, s).start()
        if s < near:
            near_sum(i, s - 1).wait_recv()
            pair[i, place(z + sign * (near - s))] = total(i, z + sign * (near - s), far + s - 1)
            near_sum(i, s).start()
        if s == far - 1:
            start_state(i)

    def update(i):
        far_sum(i, far - 1).wait_recv()
        near_sum(i, near - 1).wait_recv()
        g = total(i, z, far - 1, far + near - 1)
        g_out[i] = g
        g = g.astype(F32)
        wait_state(i)
        s = lax.rem(i, 2)
        w_new[i] = adamw(w_new[i].astype(F32), state[s, 0], state[s, 1], g)[0]
        far_ring(i, 0).start()
        near_ring(i, 0).start()
        side(i, 0).start()
        keep(i).start()

    def gather(s, i):
        far_came(i, s - 1).wait_recv()
        if s < far:
            far_ring(i, s).start()
        side(i, s).start()
        if s <= near:
            near_came(i, s - 1).wait_recv()
            if s < near:
                near_ring(i, s).start()
            side(i, far + s).start()

    def drain(i):
        for s in range(far):
            far_sum(i, s).wait_send()
            far_ring(i, s).wait_send()
        for s in range(near):
            near_sum(i, s).wait_send()
            near_ring(i, s).wait_send()
        for j in range(chips):
            side(i, j).wait_send()
            side_came(i, j).wait_recv()
        keep(i).wait()

    stages = [multiply, first]
    stages += [functools.partial(onward, s) for s in range(1, far)]
    stages += [update]
    stages += [functools.partial(gather, s) for s in range(1, far + 1)]
    stages += [drain]

    def tick(t, _):
        for offset in reversed(range(len(stages))):
            i = t - offset

            @pl.when((i >= 0) & (i < chunks))
            def _(i=i, stage=stages[offset]):
                stage(i)

            if offset == far + 1:
                extra(2 * (t - early))
        extra(2 * (t - early) + 1)
        return 0

    lax.fori_loop(0, chunks + len(stages) - 1, tick, 0)


def exchange(left, top, low, h, weights, m, v, n):
    layers, _, d, tokens = left.shape
    per = left.shape[1] - 1
    rows = d // n
    chips = n // CORES
    hops = chips - 1
    chunks = layers * 3 * per
    tile = min(tokens, 256)
    wide = 256 if d % 256 == 0 else d
    anywhere, vmem = pl.BlockSpec(memory_space=pl.ANY), pl.BlockSpec(memory_space=pltpu.VMEM)
    sems = lambda *shape: pltpu.SemaphoreType.DMA(shape)
    slots = chips // 2 + 2
    return pl.pallas_call(
        functools.partial(exchange_kernel, n, layers, per, wide, slots, tile, 3),
        in_specs=[anywhere] * 13,
        out_specs=[anywhere, vmem, anywhere],
        out_shape=[
            jax.ShapeDtypeStruct((chunks, n, rows, d), BF16),
            jax.ShapeDtypeStruct((chunks, rows, d), BF16),
            jax.ShapeDtypeStruct((2 * per + 1, tokens, d), BF16),
        ],
        scratch_shapes=[
            pltpu.VMEM((2, d, tokens), BF16),
            pltpu.VMEM((2, tokens, d), BF16),
            pltpu.VMEM((slots, CORES, chips, rows, d), BF16),
            pltpu.VMEM((chunks, chips, rows, d), BF16),
            pltpu.VMEM((chunks, hops, rows, d), BF16),
            pltpu.VMEM((2, 2, rows, d), F32),
            pltpu.VMEM((chunks, rows, d), BF16),
            pltpu.VMEM((2 * per, d, d), BF16),
            pltpu.VMEM((2 * per, tile, d), BF16),
            pltpu.VMEM((2, per, tile, d), F32),
            pltpu.VMEM((3, tile, d), BF16),
            sems(2, 2),
            sems(2, 3),
            sems(chunks),
            sems(chunks),
            sems(chunks, hops),
            sems(chunks, hops),
            sems(chunks, hops),
            sems(chunks, hops),
            sems(chunks, chips),
            sems(chunks, chips),
            sems(chunks),
            sems(2 * per),
            sems(4),
            sems(2),
        ],
        compiler_params=pltpu.CompilerParams(collective_id=0, has_side_effects=True, vmem_limit_bytes=VMEM_LIMIT),
        name="exchange",
    )(left, top, low, h, *weights, *m, *v)


def unpack_kernel(*refs):
    chunks, sums, m_in, v_in = refs[0:3], refs[3:6], refs[6:9], refs[9:12]
    (down_out, gate_out, up_out), m_out, v_out = refs[12:15], refs[15:18], refs[18:21]
    down_out[0, :, 0] = chunks[0][0]
    gate_out[0] = chunks[1][0].reshape(gate_out.shape[1:])
    up_out[0] = chunks[2][0].reshape(up_out.shape[1:])
    for kind in range(3):
        _, m_out[kind][...], v_out[kind][...] = adamw(0.0, m_in[kind][...], v_in[kind][...], sums[kind][...].astype(F32))


def unpack(new, g, m, v, shape, n):
    layers, d, ff = shape
    per, rows = ff // d, d // n
    number = lambda l, c, kind: (layers - 1 - l) * 3 * per + kind * per + c
    chunk = lambda kind: pl.BlockSpec((1, n, rows, d), lambda l, c: (number(l, c, kind), 0, 0, 0))
    sums = lambda kind: pl.BlockSpec((1, rows, d), lambda l, c: (number(l, c, kind), 0, 0))
    wide = lambda height: pl.BlockSpec((1, height, d), lambda l, c: (l, 0, c))
    moments = [pl.BlockSpec((1, rows, d), lambda l, c: (l, c, 0)), wide(rows), wide(rows)] * 2
    down, *rest = pl.pallas_call(
        unpack_kernel,
        grid=(layers, per),
        in_specs=[*(chunk(kind) for kind in range(3)), *(sums(kind) for kind in range(3)), *moments],
        out_specs=[pl.BlockSpec((1, n, 1, rows, d), lambda l, c: (l, 0, c, 0, 0)), wide(d), wide(d), *moments],
        out_shape=[
            jax.ShapeDtypeStruct((layers, n, per, rows, d), BF16),
            *[jax.ShapeDtypeStruct((layers, d, ff), BF16)] * 2,
            *(jax.ShapeDtypeStruct(t.shape, F32) for t in (*m, *v)),
        ],
        compiler_params=pltpu.CompilerParams(vmem_limit_bytes=VMEM_LIMIT),
        name="unpack",
    )(new, new, new, g, g, g, *m, *v)
    return down.reshape(layers, ff, d), *rest


def solution(mesh):
    n = mesh.shape["dp"]

    def of_a_device(x, dy, wg, wu, wd, mg, mu, md, vg, vu, vd):
        layers, d, ff = wg.shape
        tokens = x.shape[1]
        left, top, low, h = chain(x[0], dy[0], wg, wu, wd, n, min(tokens, 256))
        m, v = (md, mg, mu), (vd, vg, vu)
        new, g, _ = exchange(left, top, low, h, (wd, wg, wu), m, v, n)
        down, gate, up, md, mg, mu, vd, vg, vu = unpack(new, g, m, v, (layers, d, ff), n)
        return gate, up, down, mg, mu, md, vg, vu, vd

    data, whole, part, groups, both = P(("rep", "dp")), P(), P(None, "dp"), P("rep"), P("rep", "dp")
    return jax.shard_map(
        of_a_device,
        mesh=mesh,
        in_specs=(data, data, *[whole] * 3, *[part] * 6),
        out_specs=(*[groups] * 3, *[both] * 6),
        check_vma=False,
    )
```

```python
import functools

import jax
import jax.numpy as jnp
from jax import lax
from jax.experimental import pallas as pl
from jax.experimental.pallas import tpu as pltpu
from jax.sharding import PartitionSpec as P

CORES = 2
F32, BF16 = jnp.float32, jnp.bfloat16
VMEM_LIMIT = 67_043_328


def dot(a, b):
    return lax.dot_general(a, b, (((1,), (0,)), ((), ())), preferred_element_type=F32)


def dot_nt(a, b):
    return lax.dot_general(a, b, (((1,), (1,)), ((), ())), preferred_element_type=F32)


def silu_back(gate, up, dact):
    sig = jax.nn.sigmoid(gate)
    silu = gate * sig
    return (dact * up * (sig + silu * (1.0 - sig))).astype(BF16), (dact * silu).astype(BF16)


def adamw(w, m, v, g):
    m = 0.9 * m + 0.1 * g
    v = 0.95 * v + 0.05 * g * g
    return (w - 0.02 * (m * lax.rsqrt(v + 1e-8) + 0.1 * w)).astype(BF16), m, v


def chain_kernel(layers, blocks, x_ref, dy_ref, *refs):
    weights_hbm, (left_ref, right_ref, low_ref, h_ref), weights, sem = refs[:3], refs[3:7], refs[7:10], refs[10]
    wg_ref, wu_ref, wd_ref = weights
    d = x_ref.shape[1]
    per = wg_ref.shape[2] // d
    rows = d // blocks

    def fetch(l, which):
        return pltpu.make_async_copy(weights_hbm[which].at[l], weights[which].at[l], sem.at[l, which])

    def body(at_first):
        wait = lambda l, which: fetch(l, which).wait() if at_first else None
        if at_first:
            for l in range(layers):
                for which in range(3):
                    fetch(l, which).start()
        h = x_ref[...]
        for l in range(layers):
            wide = h.astype(F32)
            scale = lax.rsqrt(jnp.mean(wide * wide, -1, keepdims=True) + 1e-6)
            a = wide * scale
            left_ref[l, per] = a.T.astype(BF16)
            a = a.astype(BF16)
            wait(l, 0)
            wait(l, 1)
            parts, out = [], None
            for c in range(per):
                cut = slice(c * d, (c + 1) * d)
                gate, up = dot(a, wg_ref[l, :, cut]), dot(a, wu_ref[l, :, cut])
                act = jax.nn.sigmoid(gate) * gate * up
                turned = act.T.astype(BF16)
                for g in range(blocks):
                    j, p = divmod(c * blocks + g, per)
                    left_ref[l, p, j * rows : (j + 1) * rows, :] = turned[g * rows : (g + 1) * rows, :]
                if l < layers - 1:
                    low_ref[0, c], low_ref[1, c] = gate, up
                    if c == 0:
                        wait(l, 2)
                    term = dot(act.astype(BF16), wd_ref[l, cut, :])
                    out = term if out is None else out + term
                else:
                    parts.append((gate, up))
            if l < layers - 1:
                h = (wide + out.astype(BF16).astype(F32)).astype(BF16)
                h_ref[...] = h
        dh = dy_ref[...]
        right_ref[0] = dh
        wait(layers - 1, 2)
        for c, (gate, up) in enumerate(parts):
            dact = dot_nt(dh, wd_ref[layers - 1, c * d : (c + 1) * d, :]).astype(BF16).astype(F32)
            right_ref[1 + c], right_ref[1 + per + c] = silu_back(gate, up, dact)

    step = pl.program_id(0)
    pl.when(step == 0)(lambda: body(True))
    pl.when(step > 0)(lambda: body(False))


def chain(x, dy, wg, wu, wd, blocks, tile):
    layers, d, ff = wg.shape
    tokens = x.shape[0]
    per = ff // d
    tokens_by = pl.BlockSpec((tile, d), lambda t: (t, 0))
    return pl.pallas_call(
        functools.partial(chain_kernel, layers, blocks),
        grid=(tokens // tile,),
        in_specs=[tokens_by, tokens_by, *[pl.BlockSpec(memory_space=pl.ANY)] * 3],
        out_specs=[
            pl.BlockSpec((layers, per + 1, d, tile), lambda t: (0, 0, 0, t)),
            pl.BlockSpec((2 * per + 1, tile, d), lambda t: (0, t, 0)),
            pl.BlockSpec((2, per, tile, d), lambda t: (0, 0, t, 0)),
            tokens_by,
        ],
        out_shape=[
            jax.ShapeDtypeStruct((layers, per + 1, d, tokens), BF16),
            jax.ShapeDtypeStruct((2 * per + 1, tokens, d), BF16),
            jax.ShapeDtypeStruct((2, per, tokens, d), F32),
            jax.ShapeDtypeStruct((tokens, d), BF16),
        ],
        scratch_shapes=[*(pltpu.VMEM(w.shape, BF16) for w in (wg, wu, wd)), pltpu.SemaphoreType.DMA((layers, 3))],
        compiler_params=pltpu.CompilerParams(vmem_limit_bytes=VMEM_LIMIT, dimension_semantics=("arbitrary",)),
        name="chain",
    )(x, dy, wg, wu, wd)


def exchange_kernel(n, layers, per, wide, slots, tile, *refs):
    (left_hbm, top_hbm, low_hbm, h_hbm, wd_hbm, wg_hbm, wu_hbm, *rest) = refs
    m_hbm, v_hbm, new_hbm, g_out, right_hbm = rest[0:3], rest[3:6], rest[6], rest[7], rest[8]
    (lbuf, rbuf, own, pair, got, state, w_new, w_tile, t_tile, g_tile, s_tile, load_sem, state_sem, pair_send, pair_recv,
     sum_send, sum_recv, ring_send, ring_recv, side_send, side_recv, keep_sem, w_sem, in_sem, out_sem) = rest[9:]
    weights = (wd_hbm, wg_hbm, wu_hbm)
    chips = n // CORES
    far = chips // 2
    near = chips - 1 - far
    d = rbuf.shape[2]
    rows = d // n
    per_layer = 3 * per
    chunks = layers * per_layer
    me = lax.axis_index("dp")
    z, k = lax.div(me, CORES), lax.rem(me, CORES)
    sign = 1 - 2 * k
    at = lambda chip: {"dp": lax.rem(chip + 2 * chips, chips) * CORES + k}
    place = lambda chip: lax.rem(chip + 2 * chips, chips)
    fore, back, mate = at(z + sign), at(z - sign), {"dp": z * CORES + 1 - k}

    def split(i):
        layer = layers - 1 - lax.div(i, per_layer)
        q = lax.rem(i, per_layer)
        kind = lax.div(q, per)
        inner = lax.div(kind + 1, 2)
        return layer, kind, lax.rem(q, per), (1 - inner) * q + inner * per, inner * (q - per + 1)

    def start_loads(i):
        layer, _, _, of_left, of_right = split(i)
        s = lax.rem(i, 2)
        pltpu.make_async_copy(left_hbm.at[layer, of_left], lbuf.at[s], load_sem.at[s, 0]).start()
        for low, right in enumerate((top_hbm, right_hbm)):

            @pl.when((i >= per_layer) == (low == 1))
            def _(right=right):
                pltpu.make_async_copy(right.at[of_right], rbuf.at[s], load_sem.at[s, 1]).start()

    def wait_loads(i):
        s = lax.rem(i, 2)
        pltpu.make_async_copy(left_hbm.at[0, 0], lbuf.at[s], load_sem.at[s, 0]).wait()
        pltpu.make_async_copy(top_hbm.at[0], rbuf.at[s], load_sem.at[s, 1]).wait()

    def start_state(i):
        layer, kind, part, _, _ = split(i)
        s = lax.rem(i, 2)
        for which in range(3):

            @pl.when(kind == which)
            def _(which=which):
                if which == 0:
                    first_row = pl.multiple_of(me * (per * rows) + part * rows, rows)
                    w_cut = (layer, pl.ds(first_row, rows), slice(None))
                    cut = (layer, pl.ds(pl.multiple_of(part * rows, rows), rows), slice(None))
                else:
                    columns = pl.ds(pl.multiple_of(part * d, d), d)
                    w_cut = (layer, pl.ds(pl.multiple_of(me * rows, rows), rows), columns)
                    cut = (layer, slice(None), columns)
                pltpu.make_async_copy(weights[which].at[w_cut], w_new.at[i], state_sem.at[s, 0]).start()
                pltpu.make_async_copy(m_hbm[which].at[cut], state.at[s, 0], state_sem.at[s, 1]).start()
                pltpu.make_async_copy(v_hbm[which].at[cut], state.at[s, 1], state_sem.at[s, 2]).start()

    def wait_state(i):
        s = lax.rem(i, 2)
        pltpu.make_async_copy(wg_hbm.at[0, 0:rows, 0:d], w_new.at[i], state_sem.at[s, 0]).wait()
        for j, moment in enumerate((m_hbm[1], v_hbm[1])):
            pltpu.make_async_copy(moment.at[0, :, 0:d], state.at[s, j], state_sem.at[s, 1 + j]).wait()

    def remote(src, dst, send, recv, device):
        return pltpu.make_async_remote_copy(
            src_ref=src, dst_ref=dst, send_sem=send, recv_sem=recv, device_id=device, device_id_type=pl.DeviceIdType.MESH
        )

    tiles = top_hbm.shape[1] // tile

    def tokens_of(e):
        return pl.ds(pl.multiple_of(lax.rem(e, tiles) * tile, tile), tile)

    def top_weights():
        return [
            pltpu.make_async_copy(w.at[layers - 1, :, c * d : (c + 1) * d], w_tile.at[j * per + c], w_sem.at[j * per + c])
            for j, w in enumerate((wg_hbm, wu_hbm))
            for c in range(per)
        ]

    def low_weights():
        return [pltpu.make_async_copy(wd_hbm.at[0, c * d : (c + 1) * d, :], w_tile.at[c], w_sem.at[c]) for c in range(per)]

    def top_inputs(e):
        cut = tokens_of(e)
        return (
            pltpu.make_async_copy(top_hbm.at[1:, cut, :], t_tile, in_sem.at[0]),
            pltpu.make_async_copy(top_hbm.at[0, cut, :], s_tile.at[0], in_sem.at[1]),
            pltpu.make_async_copy(h_hbm.at[cut, :], s_tile.at[1], in_sem.at[2]),
        )

    def low_inputs(e):
        cut = tokens_of(e)
        return (
            pltpu.make_async_copy(low_hbm.at[:, :, cut, :], g_tile, in_sem.at[3]),
            pltpu.make_async_copy(right_hbm.at[0, cut, :], s_tile.at[0], in_sem.at[1]),
        )

    def top_result(e):
        return pltpu.make_async_copy(s_tile.at[2], right_hbm.at[0, tokens_of(e), :], out_sem.at[0])

    def low_result(e):
        return pltpu.make_async_copy(t_tile, right_hbm.at[1:, tokens_of(e), :], out_sem.at[1])

    def top_step(e):
        @pl.when(e == 0)
        def _():
            for copy in top_weights():
                copy.wait()

        @pl.when(e > 0)
        def _():
            top_result(e - 1).wait()

        for copy in top_inputs(e):
            copy.wait()
        da = dot_nt(t_tile[0], w_tile[0])
        for c in range(1, 2 * per):
            da = da + dot_nt(t_tile[c], w_tile[c])
        da = da.astype(BF16).astype(F32)
        wide = s_tile[1].astype(F32)
        scale = lax.rsqrt(jnp.mean(wide * wide, -1, keepdims=True) + 1e-6)
        mean = jnp.mean(wide * da, -1, keepdims=True)
        dwide = da * scale - wide * (scale * scale * scale * mean)
        s_tile[2] = (s_tile[0].astype(F32) + dwide.astype(BF16).astype(F32)).astype(BF16)
        top_result(e).start()

        @pl.when(e < tiles - 1)
        def _():
            for copy in top_inputs(e + 1):
                copy.start()

        @pl.when(e == tiles - 1)
        def _():
            for copy in (*low_weights(), *low_inputs(0)):
                copy.start()

    def low_step(e):
        @pl.when(e == 0)
        def _():
            top_result(tiles - 1).wait()
            for copy in low_weights():
                copy.wait()

        @pl.when(e > 0)
        def _():
            low_result(e - 1).wait()

        @pl.when(e < tiles)
        def _():
            for copy in low_inputs(e):
                copy.wait()
            for c in range(per):
                dact = dot_nt(s_tile[0], w_tile[c]).astype(BF16).astype(F32)
                t_tile[c], t_tile[per + c] = silu_back(g_tile[0, c], g_tile[1, c], dact)
            low_result(e).start()

        @pl.when(e < tiles - 1)
        def _():
            for copy in low_inputs(e + 1):
                copy.start()

    def lower(t, place):
        turn = per_layer - 1
        if place != 1:
            e = 2 * (t - (turn - tiles // 2)) + place // 2
            pl.when((e >= 0) & (e < tiles))(lambda: top_step(e))
        e_low = 3 * (t - turn) + place
        pl.when((e_low >= 0) & (e_low <= tiles))(lambda: low_step(e_low))

    start_loads(0)
    barrier = pltpu.get_barrier_semaphore()
    for device in (fore, back, mate):
        pl.semaphore_signal(barrier, inc=1, device_id=device, device_id_type=pl.DeviceIdType.MESH)
    pl.semaphore_wait(barrier, 3)

    def to_mate(i):
        return remote(own.at[lax.rem(i, slots), 1 - k], pair.at[i], pair_send.at[i], pair_recv.at[i], mate)

    def far_sum(i, s):
        return remote(pair.at[i, place(z - sign * (far - s))], got.at[i, s], sum_send.at[i, s], sum_recv.at[i, s], back)

    def near_sum(i, s):
        j = far + s
        return remote(pair.at[i, place(z + sign * (near - s))], got.at[i, j], sum_send.at[i, j], sum_recv.at[i, j], fore)

    def block(i, chip, core):
        return new_hbm.at[i, place(chip) * CORES + core]

    def far_ring(i, s):
        src = w_new.at[i] if s == 0 else block(i, z - sign * s, k)
        return remote(src, block(i, z - sign * s, k), ring_send.at[i, s], ring_recv.at[i, s], fore)

    def near_ring(i, s):
        src = w_new.at[i] if s == 0 else block(i, z + sign * s, k)
        return remote(src, block(i, z + sign * s, k), ring_send.at[i, far + s], ring_recv.at[i, far + s], back)

    def far_came(i, s):
        dst = block(i, z - sign * (s + 1), k)
        return remote(dst, dst, ring_send.at[i, s], ring_recv.at[i, s], fore)

    def near_came(i, s):
        dst = block(i, z + sign * (s + 1), k)
        return remote(dst, dst, ring_send.at[i, far + s], ring_recv.at[i, far + s], back)

    def side(i, j):
        offset = 0 if j == 0 else (-j if j <= far else j - far)
        src = w_new.at[i] if j == 0 else block(i, z + sign * offset, k)
        return remote(src, block(i, z + sign * offset, k), side_send.at[i, j], side_recv.at[i, j], mate)

    def side_came(i, j):
        offset = 0 if j == 0 else (-j if j <= far else j - far)
        dst = block(i, z - sign * offset, 1 - k)
        return remote(dst, dst, side_send.at[i, j], side_recv.at[i, j], mate)

    def keep(i):
        return pltpu.make_async_copy(w_new.at[i], block(i, z, k), keep_sem.at[i])

    def multiply(i):
        s, slot = lax.rem(i, 2), lax.rem(i, slots)

        @pl.when(i + 1 < chunks)
        def _():
            start_loads(i + 1)

        wait_loads(i)

        def columns(c, _):
            cut = pl.ds(pl.multiple_of(c * wide, wide), wide)
            out = dot(lbuf[s], rbuf[s, :, cut]).astype(BF16).reshape(chips, CORES, rows, wide)
            for core in range(CORES):
                own[slot, core, :, :, cut] = out[:, core]
            return 0

        lax.fori_loop(0, d // wide, columns, 0)
        to_mate(i).start()

    def total(i, chip, *others):
        j = place(chip)
        out = own[lax.rem(i, slots), k, j].astype(F32) + pair[i, j].astype(F32)
        for other in others:
            out = out + got[i, other].astype(F32)
        return out.astype(BF16)

    def first(i):
        to_mate(i).wait()
        pair[i, place(z - sign * far)] = total(i, z - sign * far)
        far_sum(i, 0).start()
        pair[i, place(z + sign * near)] = total(i, z + sign * near)
        near_sum(i, 0).start()

    def onward(s, i):
        far_sum(i, s - 1).wait_recv()
        pair[i, place(z - sign * (far - s))] = total(i, z - sign * (far - s), s - 1)
        far_sum(i, s).start()
        if s < near:
            near_sum(i, s - 1).wait_recv()
            pair[i, place(z + sign * (near - s))] = total(i, z + sign * (near - s), far + s - 1)
            near_sum(i, s).start()
        if s == far - 1:
            start_state(i)

    def update(i):
        far_sum(i, far - 1).wait_recv()
        near_sum(i, near - 1).wait_recv()
        g = total(i, z, far - 1, far + near - 1)
        g_out[i] = g
        g = g.astype(F32)
        wait_state(i)
        s = lax.rem(i, 2)
        w_new[i] = adamw(w_new[i].astype(F32), state[s, 0], state[s, 1], g)[0]
        far_ring(i, 0).start()
        near_ring(i, 0).start()
        side(i, 0).start()
        keep(i).start()

    def gather(s, i):
        far_came(i, s - 1).wait_recv()
        if s < far:
            far_ring(i, s).start()
        side(i, s).start()
        if s <= near:
            near_came(i, s - 1).wait_recv()
            if s < near:
                near_ring(i, s).start()
            side(i, far + s).start()

    def drain(i):
        for s in range(far):
            far_sum(i, s).wait_send()
            far_ring(i, s).wait_send()
        for s in range(near):
            near_sum(i, s).wait_send()
            near_ring(i, s).wait_send()
        for j in range(chips):
            side(i, j).wait_send()
            side_came(i, j).wait_recv()
        keep(i).wait()

    stages = [multiply, first]
    stages += [functools.partial(onward, s) for s in range(1, far)]
    stages += [update]
    stages += [functools.partial(gather, s) for s in range(1, far + 1)]

    def tick(t, _):
        @pl.when(t == 1)
        def _():
            for copy in (*top_weights(), *top_inputs(0)):
                copy.start()

        for offset in reversed(range(len(stages))):
            i = t - offset

            @pl.when((i >= 0) & (i < chunks))
            def _(i=i, stage=stages[offset]):
                stage(i)

            if offset == far + 1:
                lower(t, 0)
            if offset == 1:
                lower(t, 1)
        lower(t, 2)
        i = t - len(stages)
        pl.when((i >= 0) & (i < chunks))(lambda: drain(i))
        return 0

    lax.fori_loop(0, chunks + len(stages), tick, 0)


def exchange(left, top, low, h, weights, m, v, n):
    layers, _, d, tokens = left.shape
    per = left.shape[1] - 1
    rows = d // n
    chips = n // CORES
    hops = chips - 1
    chunks = layers * 3 * per
    tile = min(tokens, 256)
    wide = 256 if d % 256 == 0 else d
    anywhere, vmem = pl.BlockSpec(memory_space=pl.ANY), pl.BlockSpec(memory_space=pltpu.VMEM)
    sems = lambda *shape: pltpu.SemaphoreType.DMA(shape)
    slots = chips // 2 + 2
    return pl.pallas_call(
        functools.partial(exchange_kernel, n, layers, per, wide, slots, tile),
        in_specs=[anywhere] * 13,
        out_specs=[anywhere, vmem, anywhere],
        out_shape=[
            jax.ShapeDtypeStruct((chunks, n, rows, d), BF16),
            jax.ShapeDtypeStruct((chunks, rows, d), BF16),
            jax.ShapeDtypeStruct((2 * per + 1, tokens, d), BF16),
        ],
        scratch_shapes=[
            pltpu.VMEM((2, d, tokens), BF16),
            pltpu.VMEM((2, tokens, d), BF16),
            pltpu.VMEM((slots, CORES, chips, rows, d), BF16),
            pltpu.VMEM((chunks, chips, rows, d), BF16),
            pltpu.VMEM((chunks, hops, rows, d), BF16),
            pltpu.VMEM((2, 2, rows, d), F32),
            pltpu.VMEM((chunks, rows, d), BF16),
            pltpu.VMEM((2 * per, d, d), BF16),
            pltpu.VMEM((2 * per, tile, d), BF16),
            pltpu.VMEM((2, per, tile, d), F32),
            pltpu.VMEM((3, tile, d), BF16),
            sems(2, 2),
            sems(2, 3),
            sems(chunks),
            sems(chunks),
            sems(chunks, hops),
            sems(chunks, hops),
            sems(chunks, hops),
            sems(chunks, hops),
            sems(chunks, chips),
            sems(chunks, chips),
            sems(chunks),
            sems(2 * per),
            sems(4),
            sems(2),
        ],
        compiler_params=pltpu.CompilerParams(collective_id=0, has_side_effects=True, vmem_limit_bytes=VMEM_LIMIT),
        name="exchange",
    )(left, top, low, h, *weights, *m, *v)


def unpack_kernel(*refs):
    chunks, sums, m_in, v_in = refs[0:3], refs[3:6], refs[6:9], refs[9:12]
    (down_out, gate_out, up_out), m_out, v_out = refs[12:15], refs[15:18], refs[18:21]
    down_out[0, :, 0] = chunks[0][0]
    gate_out[0] = chunks[1][0].reshape(gate_out.shape[1:])
    up_out[0] = chunks[2][0].reshape(up_out.shape[1:])
    for kind in range(3):
        _, m_out[kind][...], v_out[kind][...] = adamw(0.0, m_in[kind][...], v_in[kind][...], sums[kind][...].astype(F32))


def unpack(new, g, m, v, shape, n):
    layers, d, ff = shape
    per, rows = ff // d, d // n
    halves = 1
    number = lambda l, c, kind: (layers - 1 - l) * 3 * per + kind * per + c
    chunk = lambda kind: pl.BlockSpec((1, n // halves, rows, d), lambda l, c, k: (number(l, c, kind), k, 0, 0))
    sums = lambda kind: pl.BlockSpec((1, rows, d), lambda l, c, k: (number(l, c, kind), 0, 0))
    wide = pl.BlockSpec((1, d // halves, d), lambda l, c, k: (l, k, c))
    own = pl.BlockSpec((1, rows, d), lambda l, c, k: (l, 0, c))
    moments = [pl.BlockSpec((1, rows, d), lambda l, c, k: (l, c, 0)), own, own] * 2
    down, *rest = pl.pallas_call(
        unpack_kernel,
        grid=(layers, per, halves),
        in_specs=[*(chunk(kind) for kind in range(3)), *(sums(kind) for kind in range(3)), *moments],
        out_specs=[pl.BlockSpec((1, n // halves, 1, rows, d), lambda l, c, k: (l, k, c, 0, 0)), wide, wide, *moments],
        out_shape=[
            jax.ShapeDtypeStruct((layers, n, per, rows, d), BF16),
            *[jax.ShapeDtypeStruct((layers, d, ff), BF16)] * 2,
            *(jax.ShapeDtypeStruct(t.shape, F32) for t in (*m, *v)),
        ],
        compiler_params=pltpu.CompilerParams(vmem_limit_bytes=VMEM_LIMIT),
        name="unpack",
    )(new, new, new, g, g, g, *m, *v)
    return down.reshape(layers, ff, d), *rest


def solution(mesh):
    n = mesh.shape["dp"]

    def of_a_device(x, dy, wg, wu, wd, mg, mu, md, vg, vu, vd):
        layers, d, ff = wg.shape
        tokens = x.shape[1]
        left, top, low, h = chain(x[0], dy[0], wg, wu, wd, n, min(tokens, 256))
        m, v = (md, mg, mu), (vd, vg, vu)
        new, g, _ = exchange(left, top, low, h, (wd, wg, wu), m, v, n)
        down, gate, up, md, mg, mu, vd, vg, vu = unpack(new, g, m, v, (layers, d, ff), n)
        return gate, up, down, mg, mu, md, vg, vu, vd

    data, whole, part, groups, both = P(("rep", "dp")), P(), P(None, "dp"), P("rep"), P("rep", "dp")
    return jax.shard_map(
        of_a_device,
        mesh=mesh,
        in_specs=(data, data, *[whole] * 3, *[part] * 6),
        out_specs=(*[groups] * 3, *[both] * 6),
        check_vma=False,
    )
```
